8 devices in a mesh: dz: 2 (over z, y), dy: 2 (over x), dx: 2 (over core).
Axes of the slice: x: 2, y: 2, z: 1, core: 2. Of those that a mesh axis runs over, the one named last changes fastest.
Arguments:
- x: bfloat16 [32768, 1280], P(('dx', 'dy', 'dz'))
- g: bfloat16 [32768, 1280], P(('dx', 'dy', 'dz'))
- w1: bfloat16 [1280, 5120], replicated
- w2: bfloat16 [5120, 1280], replicated
- w3: bfloat16 [1280, 5120], replicated
- w4: bfloat16 [5120, 1280], replicated
- m1: float32 [1280, 5120], P(('dx', 'dy', 'dz'))
- m2: float32 [5120, 1280], P(('dx', 'dy', 'dz'))
- m3: float32 [1280, 5120], P(('dx', 'dy', 'dz'))
- m4: float32 [5120, 1280], P(('dx', 'dy', 'dz'))
Outputs:
- output 1: bfloat16 [32768, 1280], P(('dx', 'dy', 'dz'))
- output 2: bfloat16 [1280, 5120], replicated
- output 3: bfloat16 [5120, 1280], replicated
- output 4: bfloat16 [1280, 5120], replicated
- output 5: bfloat16 [5120, 1280], replicated
- output 6: float32 [1280, 5120], P(('dx', 'dy', 'dz'))
- output 7: float32 [5120, 1280], P(('dx', 'dy', 'dz'))
- output 8: float32 [1280, 5120], P(('dx', 'dy', 'dz'))
- output 9: float32 [5120, 1280], P(('dx', 'dy', 'dz'))
All inputs are finite; a program needn't handle non-finite values.
Results may differ from the reference program's by a relative error of at most 0.0121537.
Values are sent between devices in bfloat16 or wider.
A program may use at most 1 GiB of HBM per device.

```python
import jax
import jax.numpy as jnp
from jax import lax

D = 1280
F = 5120
TOKENS_DEV = 4096
DEVICES = 8
TOKENS = TOKENS_DEV * DEVICES
LR = 0.0005
MU = 0.9


def setup_inputs(seed: int = 0) -> dict:
    ks = jax.random.split(jax.random.key(seed), 10)
    f32 = jnp.float32
    ms = 0.3 * (TOKENS_DEV / DEVICES) ** 0.5
    x = jax.random.normal(ks[0], (TOKENS, D), f32)
    g = jax.random.normal(ks[1], (TOKENS, D), f32)
    w1 = jax.random.normal(ks[2], (D, F), f32) * D ** -0.5
    w2 = jax.random.normal(ks[3], (F, D), f32) * F ** -0.5
    w3 = jax.random.normal(ks[4], (D, F), f32) * D ** -0.5
    w4 = jax.random.normal(ks[5], (F, D), f32) * F ** -0.5
    m1 = jax.random.normal(ks[6], (D, F), f32) * ms
    m2 = jax.random.normal(ks[7], (F, D), f32) * ms
    m3 = jax.random.normal(ks[8], (D, F), f32) * ms
    m4 = jax.random.normal(ks[9], (F, D), f32) * ms
    bf = jnp.bfloat16
    return {"x": x.astype(bf), "g": g.astype(bf), "w1": w1.astype(bf), "w2": w2.astype(bf),
            "w3": w3.astype(bf), "w4": w4.astype(bf), "m1": m1, "m2": m2, "m3": m3, "m4": m4}


def _gelu(z):
    return jax.nn.gelu(z, approximate=True)


def _gelu_grad(z, dh):
    return jax.vjp(_gelu, z.astype(jnp.float32))[1](dh.astype(jnp.float32))[0]


def _device_pass(x, g, w1, w2, w3, w4):
    f32, bf = jnp.float32, jnp.bfloat16
    z1 = jnp.dot(x, w1, preferred_element_type=f32).astype(bf)
    h1 = _gelu(z1.astype(f32)).astype(bf)
    h2 = (jnp.dot(h1, w2, preferred_element_type=f32) + x.astype(f32)).astype(bf)
    z3 = jnp.dot(h2, w3, preferred_element_type=f32).astype(bf)
    h3 = _gelu(z3.astype(f32)).astype(bf)
    s4 = jnp.dot(h3.T, g, preferred_element_type=f32)
    dh3 = jnp.dot(g, w4.T, preferred_element_type=f32).astype(bf)
    dz3 = _gelu_grad(z3, dh3).astype(bf)
    s3 = jnp.dot(h2.T, dz3, preferred_element_type=f32)
    dh2 = (jnp.dot(dz3, w3.T, preferred_element_type=f32) + g.astype(f32)).astype(bf)
    s2 = jnp.dot(h1.T, dh2, preferred_element_type=f32)
    dh1 = jnp.dot(dh2, w2.T, preferred_element_type=f32).astype(bf)
    dz1 = _gelu_grad(z1, dh1).astype(bf)
    s1 = jnp.dot(x.T, dz1, preferred_element_type=f32)
    dx = (jnp.dot(dz1, w1.T, preferred_element_type=f32) + dh2.astype(f32)).astype(bf)
    return dx, (s1, s2, s3, s4)


def reference(x, g, w1, w2, w3, w4, m1, m2, m3, m4):
    f32, bf = jnp.float32, jnp.bfloat16
    xs = x.reshape(DEVICES, TOKENS_DEV, D)
    gs = g.reshape(DEVICES, TOKENS_DEV, D)

    def step(acc, xg):
        dxd, ss = _device_pass(xg[0], xg[1], w1, w2, w3, w4)
        return tuple(a + s for a, s in zip(acc, ss)), dxd

    zeros = (jnp.zeros((D, F), f32), jnp.zeros((F, D), f32), jnp.zeros((D, F), f32), jnp.zeros((F, D), f32))
    acc, dxs = lax.scan(step, zeros, (xs, gs))
    m1n = MU * m1 + acc[0] / DEVICES
    m2n = MU * m2 + acc[1] / DEVICES
    m3n = MU * m3 + acc[2] / DEVICES
    m4n = MU * m4 + acc[3] / DEVICES
    w1n = (w1.astype(f32) - LR * m1n).astype(bf)
    w2n = (w2.astype(f32) - LR * m2n).astype(bf)
    w3n = (w3.astype(f32) - LR * m3n).astype(bf)
    w4n = (w4.astype(f32) - LR * m4n).astype(bf)
    dx = dxs.reshape(TOKENS, D)
    return (dx, w1n, w2n, w3n, w4n, m1n, m2n, m3n, m4n)
```

```python
import functools

import jax
import jax.numpy as jnp
from jax import lax
from jax.experimental import pallas as pl
from jax.experimental.pallas import tpu as pltpu
from jax.sharding import PartitionSpec as P


LR = 0.0005
MU = 0.9
DATA = ("dx", "dy", "dz")
C = 0.7978845608028654
CA = C * 0.044715
SWAP = [(0, 1), (1, 0)]
F32, BF = jnp.float32, jnp.bfloat16
VMEM = 60 * 2**20
NT = (((1,), (1,)), ((), ()))
TN = (((0,), (0,)), ((), ()))


def _tanh(z):
    z2 = z * z
    return z2, jnp.tanh(z * (C + CA * z2))


def _gelu(z):
    hz = 0.5 * z
    return hz + hz * _tanh(z)[1]


def _gelu_grad(z):
    z2, t = _tanh(z)
    return (0.5 + 0.5 * t) + ((1.0 - t * t) * z) * (0.5 * C + (1.5 * CA) * z2)


def _cost(m, k, n):
    return pl.CostEstimate(flops=2 * m * k * n, bytes_accessed=2 * (m * k + k * n + 2 * m * n), transcendentals=0)


def _params(dims):
    return pltpu.CompilerParams(vmem_limit_bytes=VMEM, dimension_semantics=("arbitrary",) * dims)


def _zh_body(sub, x_ref, w_ref, z_ref, h_ref):
    for i in range(x_ref.shape[0] // sub):
        s = pl.ds(i * sub, sub)
        z = jnp.dot(x_ref[s, :], w_ref[...], preferred_element_type=F32).astype(BF)
        z_ref[s, :] = z
        h_ref[s, :] = _gelu(z.astype(F32)).astype(BF)


def zh(x, w, bm=2048, bn=1280, sub=256):
    m, k = x.shape
    n = w.shape[1]
    out = pl.BlockSpec((bm, bn), lambda j, i: (i, j))
    return pl.pallas_call(
        functools.partial(_zh_body, sub), grid=(n // bn, m // bm),
        in_specs=[pl.BlockSpec((bm, k), lambda j, i: (i, 0)), pl.BlockSpec((k, bn), lambda j, i: (0, j))],
        out_specs=[out, out], out_shape=[jax.ShapeDtypeStruct((m, n), BF)] * 2,
        cost_estimate=_cost(m, k, n), compiler_params=_params(2))(x, w)


def _dz_body(sub, g_ref, w_ref, z_ref, o_ref):
    for i in range(g_ref.shape[0] // sub):
        s = pl.ds(i * sub, sub)
        dh = lax.dot_general(g_ref[s, :], w_ref[...], NT, preferred_element_type=F32).astype(BF)
        o_ref[s, :] = (_gelu_grad(z_ref[s, :].astype(F32)) * dh.astype(F32)).astype(BF)


def dz_half(g, w, z, half, bm=1024, bn=1280, sub=256):
    m, k = g.shape
    n = w.shape[0] // 2
    off = half * (n // bn)
    return pl.pallas_call(
        functools.partial(_dz_body, sub), grid=(n // bn, m // bm),
        in_specs=[pl.BlockSpec((bm, k), lambda j, i: (i, 0)),
                  pl.BlockSpec((bn, k), lambda j, i: (j + off, 0)),
                  pl.BlockSpec((bm, bn), lambda j, i: (i, j + off))],
        out_specs=pl.BlockSpec((bm, bn), lambda j, i: (i, j)),
        out_shape=jax.ShapeDtypeStruct((m, n), BF),
        cost_estimate=_cost(m, k, n), compiler_params=_params(2))(g, w, z)


def _back_body(sub, a_ref, b_ref, wa_ref, wb_ref, r_ref, *refs):
    o_ref = refs[-1]
    for i in range(a_ref.shape[0] // sub):
        s = pl.ds(i * sub, sub)
        acc = lax.dot_general(a_ref[s, :], wa_ref[...], NT, preferred_element_type=F32)
        acc += lax.dot_general(b_ref[s, :], wb_ref[...], NT, preferred_element_type=F32)
        o_ref[s, :] = (acc + r_ref[s, :].astype(F32)).astype(BF)


def back(a, b, w, r, pieces=1, piece=0, into=None, bm=512, sub=256):
    m, k = a.shape
    n = w.shape[0]
    steps = m // bm // pieces
    off = piece * steps
    rows = pl.BlockSpec((bm, k), lambda i: (i + off, 0))
    out = pl.BlockSpec((bm, n), lambda i: (i + off, 0))
    extra = [] if into is None else [into]
    return pl.pallas_call(
        functools.partial(_back_body, sub), grid=(steps,),
        in_specs=[rows, rows, pl.BlockSpec((n, k), lambda i: (0, 0)), pl.BlockSpec((n, k), lambda i: (0, 1)), out]
        + [pl.BlockSpec(memory_space=pl.ANY)] * len(extra),
        out_specs=out, out_shape=jax.ShapeDtypeStruct((m, n), BF),
        input_output_aliases={5: 0} if extra else {},
        cost_estimate=_cost(m // pieces, 2 * k, n), compiler_params=_params(1))(a, b, w, w, r, *extra)


def _grad_body(h_ref, a_ref, b_ref, *refs):
    s = lax.dot_general(a_ref[...], b_ref[...], TN, preferred_element_type=F32)
    refs[-1][...] = s if len(refs) == 1 else s + refs[0][...]


def grad(half, a, b, start, cols, bm, bn, recv=None):
    k = a.shape[0]
    rows = a.shape[1] // 2
    tiles = rows // bm
    out = pl.BlockSpec((bm, bn), lambda i, j, h: (i, j))
    specs = [pl.BlockSpec((k, bm), lambda i, j, h: (0, i + h[0] * tiles)),
             pl.BlockSpec((pl.Element(k), pl.Element(bn)), lambda i, j, h: (0, pl.multiple_of(start + j * bn, 128)))]
    args = [half, a, b]
    if recv is not None:
        specs.append(out)
        args.append(recv)
    return pl.pallas_call(
        _grad_body,
        grid_spec=pltpu.PrefetchScalarGridSpec(num_scalar_prefetch=1, grid=(tiles, cols // bn), in_specs=specs,
                                               out_specs=out),
        out_shape=jax.ShapeDtypeStruct((rows, cols), F32),
        cost_estimate=_cost(rows, k, cols), compiler_params=_params(2))(*args)


def _copy_body(*refs):
    refs[-1][...] = refs[0][...]


def copy(w, shape=None, half=0, into=None, steps=8):
    rows, cols = w.shape
    block = pl.BlockSpec((rows // steps, cols), lambda i: (i, 0))
    return pl.pallas_call(
        _copy_body, grid=(steps,),
        in_specs=[block] + ([] if into is None else [pl.BlockSpec(memory_space=pl.ANY)]),
        out_specs=pl.BlockSpec((rows // steps, cols), lambda i: (i, half)),
        out_shape=jax.ShapeDtypeStruct(shape or w.shape, w.dtype),
        input_output_aliases={} if into is None else {1: 0},
        cost_estimate=pl.CostEstimate(flops=rows * cols * 64, bytes_accessed=4 * rows * cols, transcendentals=0),
        compiler_params=_params(1))(w, *([] if into is None else [into]))


class Chunk:
    def __init__(self, s):
        self.j, self.k = lax.axis_index("dy"), lax.axis_index("dz")
        rows, cols = s.shape
        self.size = rows // 8, cols
        self.s = s.reshape(2, 2, 2, rows // 8, cols)
        self.out = self.cut(1 - self.j, 0, 0, (1, 2)), self.cut(0, 1 - self.k, 1, (2, 1))

    def cut(self, j, k, part, n):
        r, c = self.size
        return lax.dynamic_slice(self.s, (j, k, part, 0, 0), (*n, 1, r, c)).reshape(n[0] * n[1], r, c)

    def send(self, stage, vals):
        axes = ("dy", "dz") if stage == 1 else ("dz", "dy")
        self.flight = []
        for v, ax in zip(vals, axes):
            self.flight.append(lax.ppermute(v, ax, SWAP))

    def second(self, vals):
        j, k = self.j, self.k
        self.ra, self.rb = vals
        pick = lax.dynamic_index_in_dim
        self.out = (self.cut(j, 1 - k, 0, (1, 1)) + pick(self.ra, 1 - k, 0),
                    self.cut(1 - j, k, 1, (1, 1)) + pick(self.rb, 1 - j, 0))

    def total(self, vals):
        j, k = self.j, self.k
        pick = lax.dynamic_index_in_dim
        a = self.cut(j, k, 0, (1, 1)) + pick(self.ra, k, 0) + vals[0]
        b = self.cut(j, k, 1, (1, 1)) + pick(self.rb, j, 0) + vals[1]
        return jnp.concatenate([a[0], b[0]], axis=0)


def solution(mesh):
    ndy, ndz = mesh.shape["dy"], mesh.shape["dz"]
    n = mesh.shape["dx"] * ndy * ndz

    def dot(a, b):
        return jnp.dot(a, b, preferred_element_type=F32)

    def local(x, g, w1, w2, w3, w4, m1, m2, m3, m4):
        core = lax.axis_index("dx")
        own = core.astype(jnp.int32).reshape(1)
        other = 1 - own
        tall = dict(a=dict(start=0, cols=512, bm=640, bn=512), b=dict(start=512, cols=768, bm=640, bn=768))
        whole = dict(a=dict(start=0, cols=2560, bm=640, bn=512))
        whole["b"] = whole["a"]

        def gate(*vals):
            return lax.optimization_barrier(vals)

        def send(s):
            return lax.ppermute(s, "dx", SWAP)

        def part(layer, which, a, b, recv=None):
            half, _ = (other, "p") if recv is None else (own, "o")
            sizes = (tall if layer in "24" else whole)[which]
            return grad(half, a, b, **sizes, recv=recv)

        def update(w, m, s, start=0):
            rows, cols = s.shape
            idx = (core * ndy + lax.axis_index("dy")) * ndz + lax.axis_index("dz")
            m_new = MU * lax.slice_in_dim(m, start, start + cols, axis=1) + s / n
            w_loc = lax.dynamic_slice(w, (idx * rows, start), (rows, cols)).astype(F32)
            return (w_loc - LR * m_new).astype(BF), m_new

        def both(ca, cb, vals):
            return jnp.concatenate([ca.total(vals[:2]), cb.total(vals[2:])], axis=1)

        def gather(w):
            return lax.all_gather(w, DATA, axis=0, tiled=True)

        z1, h1 = zh(x, w1)
        h2 = (dot(h1, w2) + x.astype(F32)).astype(BF)
        z3, h3 = zh(h2, w3)

        h3, p = gate(h3, part("4", "a", h3, g))
        d4a = send(p)
        h3, p = gate(h3, part("4", "b", h3, g))
        d4b = send(p)
        c4a = Chunk(part("4", "a", h3, g, d4a))
        h3, *v = gate(h3, *c4a.out)
        c4a.send(1, v)
        c4b = Chunk(part("4", "b", h3, g, d4b))
        g_, *v = gate(g, *c4b.out)
        c4b.send(1, v)
        dza = dz_half(g_, w4, z3, 0)
        dza, *v = gate(dza, *c4a.flight, *c4b.flight)
        c4a.second(v[:2])
        c4b.second(v[2:])
        dza, *v = gate(dza, *c4a.out, *c4b.out)
        c4a.send(2, v[:2])
        c4b.send(2, v[2:])
        g_, p = gate(g_, part("3", "a", h2, dza))
        d3a = send(p)
        dzb = dz_half(g_, w4, z3, 1)
        dzb, *v = gate(dzb, *c4a.flight, *c4b.flight)
        w4l, m4n = update(w4, m4, both(c4a, c4b, v))
        dzb, w4l, m4n = gate(dzb, w4l, m4n)
        w4g = gather(w4l)
        dza, p = gate(dza, part("3", "b", h2, dzb))
        d3b = send(p)
        c3a = Chunk(part("3", "a", h2, dza, d3a))
        dzb, *v = gate(dzb, *c3a.out)
        c3a.send(1, v)
        c3b = Chunk(part("3", "b", h2, dzb, d3b))
        dzb, *v = gate(dzb, *c3b.out)
        c3b.send(1, v)
        dh2 = back(dza, dzb, w3, g)
        dh2, *v = gate(dh2, *c3a.flight, *c3b.flight)
        c3a.second(v[:2])
        c3b.second(v[2:])
        dh2, *v = gate(dh2, *c3a.out, *c3b.out)
        c3a.send(2, v[:2])
        c3b.send(2, v[2:])
        dh2, p = gate(dh2, part("2", "a", h1, dh2))
        d2a = send(p)
        p = part("2", "b", h1, dh2)
        dh2, p, *v = gate(dh2, p, *c3a.flight, *c3b.flight)
        d2b = send(p)
        w3l, m3n = update(w3, m3, both(c3a, c3b, v))
        dh2, w3l, m3n = gate(dh2, w3l, m3n)
        w3g = gather(w3l)
        c2a = Chunk(part("2", "a", h1, dh2, d2a))
        dh2, *v = gate(dh2, *c2a.out)
        c2a.send(1, v)
        c2b = Chunk(part("2", "b", h1, dh2, d2b))
        dh2, *v = gate(dh2, *c2b.out)
        c2b.send(1, v)
        dza = dz_half(dh2, w2, z1, 0)
        p = part("1", "a", x, dza)
        dh2, p, *v = gate(dh2, p, *c2a.flight, *c2b.flight)
        d1a = send(p)
        c2a.second(v[:2])
        c2b.second(v[2:])
        dh2, *v = gate(dh2, *c2a.out, *c2b.out)
        c2a.send(2, v[:2])
        c2b.send(2, v[2:])
        dzb = dz_half(dh2, w2, z1, 1)
        dzb, *v = gate(dzb, *c2a.flight, *c2b.flight)
        w2l, m2n = update(w2, m2, both(c2a, c2b, v))
        dzb, w2l, m2n = gate(dzb, w2l, m2n)
        w2g = gather(w2l)
        dza, p = gate(dza, part("1", "b", x, dzb))
        d1b = send(p)
        c1a = Chunk(part("1", "a", x, dza, d1a))
        dzb, *v = gate(dzb, *c1a.out)
        c1a.send(1, v)
        c1b = Chunk(part("1", "b", x, dzb, d1b))
        dzb, *v = gate(dzb, *c1b.out)
        c1b.send(1, v)
        top = back(dza, dzb, w1, dh2, 2, 0)
        top, *v = gate(top, *c1a.flight)
        c1a.second(v)
        top, *v = gate(top, *c1a.out)
        c1a.send(2, v)
        dx = back(dza, dzb, w1, dh2, 2, 1, top)
        dx, w4g, *v = gate(dx, w4g, *c1b.flight)
        c1b.second(v)
        w4g, *v = gate(w4g, *c1b.out)
        c1b.send(2, v)
        w4g, *v = gate(w4g, *c1a.flight)
        wa, ma = update(w1, m1, c1a.total(v))
        w4g, wa = gate(w4g, wa)
        ga = gather(wa)
        w4n = copy(w4g)
        w4n, w3g, *v = gate(w4n, w3g, *c1b.flight)
        wb, mb = update(w1, m1, c1b.total(v), start=wa.shape[1])
        w3g, wb = gate(w3g, wb)
        gb = gather(wb)
        w3n = copy(w3g)
        w3n, w2g = gate(w3n, w2g)
        w2n = copy(w2g)
        w2n, ga = gate(w2n, ga)
        half = copy(ga, w1.shape, 0)
        half, gb = gate(half, gb)
        w1n = copy(gb, w1.shape, 1, half)
        m1n = jnp.concatenate([ma, mb], axis=1)
        return (dx, w1n, w2n, w3n, w4n, m1n, m2n, m3n, m4n)

    row, rep = P(DATA, None), P()
    return jax.shard_map(local, mesh=mesh,
                         in_specs=(row, row, rep, rep, rep, rep, row, row, row, row),
                         out_specs=(row, rep, rep, rep, rep, row, row, row, row),
                         check_vma=False)
```

```python
import functools

import jax
import jax.numpy as jnp
from jax import lax
from jax.experimental import pallas as pl
from jax.experimental.pallas import tpu as pltpu
from jax.sharding import PartitionSpec as P


LR = 0.0005
MU = 0.9
DATA = ("dx", "dy", "dz")
C = 0.7978845608028654
CA = C * 0.044715
SWAP = [(0, 1), (1, 0)]
F32, BF = jnp.float32, jnp.bfloat16
CUTS = (pl.ds(0, 768), pl.ds(768, 512))
NT = (((1,), (1,)), ((), ()))
TN = (((0,), (0,)), ((), ()))


def _tanh(z):
    z2 = z * z
    return z2, jnp.tanh(z * (C + CA * z2))


def _gelu(z):
    hz = 0.5 * z
    return hz + hz * _tanh(z)[1]


def _gelu_grad(z):
    z2, t = _tanh(z)
    return (0.5 + 0.5 * t) + ((1.0 - t * t) * z) * (0.5 * C + (1.5 * CA) * z2)


def _cost(m, k, n):
    return pl.CostEstimate(flops=2 * m * k * n, bytes_accessed=2 * (m * k + k * n + 2 * m * n), transcendentals=0)


def _params(dims, mib=60):
    return pltpu.CompilerParams(vmem_limit_bytes=mib * 2**20, dimension_semantics=("arbitrary",) * dims)


def _zh_body(sub, x_ref, w_ref, z_ref, h_ref):
    for i in range(x_ref.shape[0] // sub):
        s = pl.ds(i * sub, sub)
        for c in CUTS:
            z = jnp.dot(x_ref[s, :], w_ref[:, c], preferred_element_type=F32).astype(BF)
            z_ref[s, c] = z
            h_ref[s, c] = _gelu(z.astype(F32)).astype(BF)


def zh(x, w, bm=2048, bn=1280, sub=256):
    m, k = x.shape
    n = w.shape[1]
    out = pl.BlockSpec((bm, bn), lambda j, i: (i, j))
    return pl.pallas_call(
        functools.partial(_zh_body, sub), grid=(n // bn, m // bm),
        in_specs=[pl.BlockSpec((bm, k), lambda j, i: (i, 0)), pl.BlockSpec((k, bn), lambda j, i: (0, j))],
        out_specs=[out, out], out_shape=[jax.ShapeDtypeStruct((m, n), BF)] * 2,
        cost_estimate=_cost(m, k, n), compiler_params=_params(2, 44))(x, w)


def _dz_body(sub, g_ref, w_ref, z_ref, o_ref):
    for i in range(g_ref.shape[0] // sub):
        s = pl.ds(i * sub, sub)
        for c in CUTS:
            dh = lax.dot_general(g_ref[s, :], w_ref[c, :], NT, preferred_element_type=F32).astype(BF)
            o_ref[s, c] = (_gelu_grad(z_ref[s, c].astype(F32)) * dh.astype(F32)).astype(BF)


def dz_half(g, w, z, half, bm=1024, bn=1280, sub=256):
    m, k = g.shape
    n = w.shape[0] // 2
    off = half * (n // bn)
    return pl.pallas_call(
        functools.partial(_dz_body, sub), grid=(n // bn, m // bm),
        in_specs=[pl.BlockSpec((bm, k), lambda j, i: (i, 0)),
                  pl.BlockSpec((bn, k), lambda j, i: (j + off, 0)),
                  pl.BlockSpec((bm, bn), lambda j, i: (i, j + off))],
        out_specs=pl.BlockSpec((bm, bn), lambda j, i: (i, j)),
        out_shape=jax.ShapeDtypeStruct((m, n), BF),
        cost_estimate=_cost(m, k, n), compiler_params=_params(2))(g, w, z)


def _back_body(sub, a_ref, b_ref, wa_ref, wb_ref, r_ref, *refs):
    o_ref = refs[-1]
    for i in range(a_ref.shape[0] // sub):
        s = pl.ds(i * sub, sub)
        acc = lax.dot_general(a_ref[s, :], wa_ref[...], NT, preferred_element_type=F32)
        acc += lax.dot_general(b_ref[s, :], wb_ref[...], NT, preferred_element_type=F32)
        o_ref[s, :] = (acc + r_ref[s, :].astype(F32)).astype(BF)


def back(a, b, w, r, pieces=1, piece=0, into=None, bm=512, sub=256):
    m, k = a.shape
    n = w.shape[0]
    steps = m // bm // pieces
    off = piece * steps
    rows = pl.BlockSpec((bm, k), lambda i: (i + off, 0))
    out = pl.BlockSpec((bm, n), lambda i: (i + off, 0))
    extra = [] if into is None else [into]
    return pl.pallas_call(
        functools.partial(_back_body, sub), grid=(steps,),
        in_specs=[rows, rows, pl.BlockSpec((n, k), lambda i: (0, 0)), pl.BlockSpec((n, k), lambda i: (0, 1)), out]
        + [pl.BlockSpec(memory_space=pl.ANY)] * len(extra),
        out_specs=out, out_shape=jax.ShapeDtypeStruct((m, n), BF),
        input_output_aliases={5: 0} if extra else {},
        cost_estimate=_cost(m // pieces, 2 * k, n), compiler_params=_params(1))(a, b, w, w, r, *extra)


def _grad_body(at_ref, a_ref, b_ref, *refs):
    s = lax.dot_general(a_ref[...], b_ref[...], TN, preferred_element_type=F32)
    if len(refs) == 1:
        refs[0][...] = s
        return
    r_ref, o_ref, first_ref, second_ref = refs
    o_ref[...] = s + r_ref[...]
    part = first_ref.shape[1]
    far_j, far_k = 1 - at_ref[1], 1 - at_ref[2]
    if first_ref.shape[0] == 2:
        for i in range(2):
            first_ref[i] = o_ref[pl.ds(pl.multiple_of((far_j * 2 + i) * 2 * part, 8), part), :]
            second_ref[i] = o_ref[pl.ds(pl.multiple_of((i * 2 + far_k) * 2 * part + part, 8), part), :]
    else:
        i = pl.program_id(0)

        @pl.when(i // 2 == far_j)
        def _():
            first_ref[0] = o_ref[:part, :]

        @pl.when(i % 2 == far_k)
        def _():
            second_ref[0] = o_ref[part:, :]


def grad(at, a, b, start, cols, bm, bn, mib, recv=None):
    k = a.shape[0]
    rows = a.shape[1] // 2
    tiles = rows // bm
    out = pl.BlockSpec((bm, bn), lambda i, j, t: (i, j))
    shape = jax.ShapeDtypeStruct((rows, cols), F32)
    specs = [pl.BlockSpec((k, bm), lambda i, j, t: (0, i + t[0] * tiles)),
             pl.BlockSpec((pl.Element(k), pl.Element(bn)), lambda i, j, t: (0, pl.multiple_of(start + j * bn, 128)))]
    args = [at, a, b]
    if recv is not None:
        specs.append(out)
        args.append(recv)
        if tiles == 1:
            one = two = pl.BlockSpec((2, rows // 8, bn), lambda i, j, t: (0, 0, j))
        else:
            one = pl.BlockSpec((1, rows // 8, bn), lambda i, j, t: (jnp.clip(i - 2 * (1 - t[1]), 0, 1), 0, j))
            two = pl.BlockSpec((1, rows // 8, bn), lambda i, j, t: (i // 2, 0, j))
        out = [out, one, two]
        shape = [shape] + [jax.ShapeDtypeStruct((2, rows // 8, cols), F32)] * 2
    return pl.pallas_call(
        _grad_body,
        grid_spec=pltpu.PrefetchScalarGridSpec(num_scalar_prefetch=1, grid=(tiles, cols // bn), in_specs=specs,
                                               out_specs=out),
        out_shape=shape, cost_estimate=_cost(rows, k, cols), compiler_params=_params(2, mib))(*args)


def _copy_body(*refs):
    refs[-1][...] = refs[0][...]


def copy(w, shape=None, half=0, into=None, steps=8):
    rows, cols = w.shape
    block = pl.BlockSpec((rows // steps, cols), lambda i: (i, 0))
    return pl.pallas_call(
        _copy_body, grid=(steps,),
        in_specs=[block] + ([] if into is None else [pl.BlockSpec(memory_space=pl.ANY)]),
        out_specs=pl.BlockSpec((rows // steps, cols), lambda i: (i, half)),
        out_shape=jax.ShapeDtypeStruct(shape or w.shape, w.dtype),
        input_output_aliases={} if into is None else {1: 0},
        cost_estimate=pl.CostEstimate(flops=rows * cols * 64, bytes_accessed=4 * rows * cols, transcendentals=0),
        compiler_params=_params(1))(w, *([] if into is None else [into]))


class Chunk:
    def __init__(self, parts):
        s, *self.out = parts
        self.j, self.k = lax.axis_index("dy"), lax.axis_index("dz")
        rows, cols = s.shape
        self.size = rows // 8, cols
        self.s = s.reshape(2, 2, 2, rows // 8, cols)

    def cut(self, j, k, part, n):
        r, c = self.size
        return lax.dynamic_slice(self.s, (j, k, part, 0, 0), (*n, 1, r, c)).reshape(n[0] * n[1], r, c)

    def send(self, stage, vals):
        axes = ("dy", "dz") if stage == 1 else ("dz", "dy")
        self.flight = []
        for v, ax in zip(vals, axes):
            self.flight.append(lax.ppermute(v, ax, SWAP))

    def second(self, vals):
        j, k = self.j, self.k
        self.ra, self.rb = vals
        pick = lax.dynamic_index_in_dim
        self.out = (self.cut(j, 1 - k, 0, (1, 1)) + pick(self.ra, 1 - k, 0),
                    self.cut(1 - j, k, 1, (1, 1)) + pick(self.rb, 1 - j, 0))

    def total(self, vals):
        j, k = self.j, self.k
        pick = lax.dynamic_index_in_dim
        a = self.cut(j, k, 0, (1, 1)) + pick(self.ra, k, 0) + vals[0]
        b = self.cut(j, k, 1, (1, 1)) + pick(self.rb, j, 0) + vals[1]
        return jnp.concatenate([a[0], b[0]], axis=0)


def solution(mesh):
    ndy, ndz = mesh.shape["dy"], mesh.shape["dz"]
    n = mesh.shape["dx"] * ndy * ndz

    def dot(a, b):
        return jnp.dot(a, b, preferred_element_type=F32)

    def local(x, g, w1, w2, w3, w4, m1, m2, m3, m4):
        core = lax.axis_index("dx")
        spot = [core, lax.axis_index("dy"), lax.axis_index("dz")]
        own = jnp.stack(spot).astype(jnp.int32)
        other = jnp.stack([1 - core, *spot[1:]]).astype(jnp.int32)
        tall = dict(a=dict(start=0, cols=512, bm=640, bn=512), b=dict(start=512, cols=768, bm=640, bn=768))
        whole = dict(a=dict(start=0, cols=2560, bm=640, bn=512))
        whole["b"] = whole["a"]

        def gate(*vals):
            return lax.optimization_barrier(vals)

        def send(s):
            return lax.ppermute(s, "dx", SWAP)

        def part(layer, which, a, b, recv=None):
            half, _ = (other, "p") if recv is None else (own, "o")
            sizes = (tall if layer in "24" else whole)[which]
            return grad(half, a, b, **sizes, mib=38 if layer == "4" else 60, recv=recv)

        def update(w, m, s, start=0):
            rows, cols = s.shape
            idx = (core * ndy + lax.axis_index("dy")) * ndz + lax.axis_index("dz")
            m_new = MU * lax.slice_in_dim(m, start, start + cols, axis=1) + s / n
            w_loc = lax.dynamic_slice(w, (idx * rows, start), (rows, cols)).astype(F32)
            return (w_loc - LR * m_new).astype(BF), m_new

        def both(ca, cb, vals):
            return jnp.concatenate([ca.total(vals[:2]), cb.total(vals[2:])], axis=1)

        def gather(w):
            return lax.all_gather(w, DATA, axis=0, tiled=True)

        z1, h1 = zh(x, w1)
        h2 = (dot(h1, w2) + x.astype(F32)).astype(BF)
        z3, h3 = zh(h2, w3)

        h3, p = gate(h3, part("4", "a", h3, g))
        d4a = send(p)
        h3, p = gate(h3, part("4", "b", h3, g))
        d4b = send(p)
        c4a = Chunk(part("4", "a", h3, g, d4a))
        h3, *v = gate(h3, *c4a.out)
        c4a.send(1, v)
        c4b = Chunk(part("4", "b", h3, g, d4b))
        g_, *v = gate(g, *c4b.out)
        c4b.send(1, v)
        g_, *v = gate(g_, *c4a.flight)
        c4a.second(v)
        g_, *v = gate(g_, *c4a.out)
        c4a.send(2, v)
        dza = dz_half(g_, w4, z3, 0)
        dza, *v = gate(dza, *c4b.flight)
        c4b.second(v)
        dza, *v = gate(dza, *c4b.out)
        c4b.send(2, v)
        g_, p = gate(g_, part("3", "a", h2, dza))
        d3a = send(p)
        g_, *v = gate(g_, *c4a.flight, *c4b.flight)
        w4l, m4n = update(w4, m4, both(c4a, c4b, v))
        g_, w4l, m4n = gate(g_, w4l, m4n)
        w4g = gather(w4l)
        dzb = dz_half(g_, w4, z3, 1)
        dza, p = gate(dza, part("3", "b", h2, dzb))
        d3b = send(p)
        c3a = Chunk(part("3", "a", h2, dza, d3a))
        dzb, *v = gate(dzb, *c3a.out)
        c3a.send(1, v)
        c3b = Chunk(part("3", "b", h2, dzb, d3b))
        dzb, *v = gate(dzb, *c3b.out)
        c3b.send(1, v)
        top = back(dza, dzb, w3, g, 2, 0)
        top, *v = gate(top, *c3a.flight)
        c3a.second(v)
        top, *v = gate(top, *c3a.out)
        c3a.send(2, v)
        dh2 = back(dza, dzb, w3, g, 2, 1, top)
        dh2, *v = gate(dh2, *c3b.flight)
        c3b.second(v)
        dh2, *v = gate(dh2, *c3b.out)
        c3b.send(2, v)
        dh2, p = gate(dh2, part("2", "a", h1, dh2))
        d2a = send(p)
        dh2, *v = gate(dh2, *c3a.flight, *c3b.flight)
        w3l, m3n = update(w3, m3, both(c3a, c3b, v))
        dh2, w3l, m3n = gate(dh2, w3l, m3n)
        w3g = gather(w3l)
        dh2, p = gate(dh2, part("2", "b", h1, dh2))
        d2b = send(p)
        c2a = Chunk(part("2", "a", h1, dh2, d2a))
        dh2, *v = gate(dh2, *c2a.out)
        c2a.send(1, v)
        c2b = Chunk(part("2", "b", h1, dh2, d2b))
        dh2, *v = gate(dh2, *c2b.out)
        c2b.send(1, v)
        dza = dz_half(dh2, w2, z1, 0)
        p = part("1", "a", x, dza)
        dh2, p, *v = gate(dh2, p, *c2a.flight, *c2b.flight)
        d1a = send(p)
        c2a.second(v[:2])
        c2b.second(v[2:])
        dh2, *v = gate(dh2, *c2a.out, *c2b.out)
        c2a.send(2, v[:2])
        c2b.send(2, v[2:])
        dzb = dz_half(dh2, w2, z1, 1)
        dzb, *v = gate(dzb, *c2a.flight, *c2b.flight)
        w2l, m2n = update(w2, m2, both(c2a, c2b, v))
        dzb, w2l, m2n = gate(dzb, w2l, m2n)
        w2g = gather(w2l)
        c1a = Chunk(part("1", "a", x, dza, d1a))
        dzb, *v = gate(dzb, *c1a.out)
        c1a.send(1, v)
        dza, w4g, p = gate(dza, w4g, part("1", "b", x, dzb))
        d1b = send(p)
        w4n = copy(w4g)
        dzb, d1b, w4n = gate(dzb, d1b, w4n)
        c1b = Chunk(part("1", "b", x, dzb, d1b))
        dzb, *v = gate(dzb, *c1b.out)
        c1b.send(1, v)
        dzb, *v = gate(dzb, *c1a.flight)
        c1a.second(v)
        dzb, *v = gate(dzb, *c1a.out)
        c1a.send(2, v)
        top = back(dza, dzb, w1, dh2, 2, 0)
        top, *v = gate(top, *c1a.flight)
        wa, ma = update(w1, m1, c1a.total(v))
        top, wa = gate(top, wa)
        ga = gather(wa)
        top, w3g, *v = gate(top, w3g, *c1b.flight)
        c1b.second(v)
        top, w3g, *v = gate(top, w3g, *c1b.out)
        c1b.send(2, v)
        w3n = copy(w3g)
        w3n, w2g = gate(w3n, w2g)
        w2n = copy(w2g)
        top, w2n, *v = gate(top, w2n, *c1b.flight)
        wb, mb = update(w1, m1, c1b.total(v), start=wa.shape[1])
        top, wb = gate(top, wb)
        gb = gather(wb)
        dx = back(dza, dzb, w1, dh2, 2, 1, top)
        dx, ga = gate(dx, ga)
        half = copy(ga, w1.shape, 0)
        half, gb = gate(half, gb)
        w1n = copy(gb, w1.shape, 1, half)
        m1n = jnp.concatenate([ma, mb], axis=1)
        return (dx, w1n, w2n, w3n, w4n, m1n, m2n, m3n, m4n)

    row, rep = P(DATA, None), P()
    return jax.shard_map(local, mesh=mesh,
                         in_specs=(row, row, rep, rep, rep, rep, row, row, row, row),
                         out_specs=(row, rep, rep, rep, rep, row, row, row, row),
                         check_vma=False)
```

```python
import functools

import jax
import jax.numpy as jnp
from jax import lax
from jax.experimental import pallas as pl
from jax.experimental.pallas import tpu as pltpu
from jax.sharding import PartitionSpec as P


LR = 0.0005
MU = 0.9
DATA = ("dx", "dy", "dz")
C = 0.7978845608028654
CA = C * 0.044715
SWAP = [(0, 1), (1, 0)]
F32, BF = jnp.float32, jnp.bfloat16
CUTS = (pl.ds(0, 768), pl.ds(768, 512))
NT = (((1,), (1,)), ((), ()))
TN = (((0,), (0,)), ((), ()))


def _tanh(z):
    z2 = z * z
    return z2, jnp.tanh(z * (C + CA * z2))


def _gelu(z):
    hz = 0.5 * z
    return hz + hz * _tanh(z)[1]


def _gelu_grad(z):
    z2, t = _tanh(z)
    return (0.5 + 0.5 * t) + ((1.0 - t * t) * z) * (0.5 * C + (1.5 * CA) * z2)


def _cost(m, k, n):
    return pl.CostEstimate(flops=2 * m * k * n, bytes_accessed=2 * (m * k + k * n + 2 * m * n), transcendentals=0)


def _params(dims, mib=60):
    return pltpu.CompilerParams(vmem_limit_bytes=mib * 2**20, dimension_semantics=("arbitrary",) * dims)


def _zh_body(sub, x_ref, w_ref, z_ref, h_ref):
    for i in range(x_ref.shape[0] // sub):
        s = pl.ds(i * sub, sub)
        for c in CUTS:
            z = jnp.dot(x_ref[s, :], w_ref[:, c], preferred_element_type=F32).astype(BF)
            z_ref[s, c] = z
            h_ref[s, c] = _gelu(z.astype(F32)).astype(BF)


def zh(x, w, bm=2048, bn=1280, sub=256):
    m, k = x.shape
    n = w.shape[1]
    out = pl.BlockSpec((bm, bn), lambda j, i: (i, j))
    return pl.pallas_call(
        functools.partial(_zh_body, sub), grid=(n // bn, m // bm),
        in_specs=[pl.BlockSpec((bm, k), lambda j, i: (i, 0)), pl.BlockSpec((k, bn), lambda j, i: (0, j))],
        out_specs=[out, out], out_shape=[jax.ShapeDtypeStruct((m, n), BF)] * 2,
        cost_estimate=_cost(m, k, n), compiler_params=_params(2, 44))(x, w)


def _dz_body(sub, g_ref, w_ref, z_ref, o_ref):
    for i in range(g_ref.shape[0] // sub):
        s = pl.ds(i * sub, sub)
        for c in CUTS:
            dh = lax.dot_general(g_ref[s, :], w_ref[c, :], NT, preferred_element_type=F32).astype(BF)
            o_ref[s, c] = (_gelu_grad(z_ref[s, c].astype(F32)) * dh.astype(F32)).astype(BF)


def dz_half(g, w, z, half, bm=1024, bn=1280, sub=256):
    m, k = g.shape
    n = w.shape[0] // 2
    off = half * (n // bn)
    return pl.pallas_call(
        functools.partial(_dz_body, sub), grid=(n // bn, m // bm),
        in_specs=[pl.BlockSpec((bm, k), lambda j, i: (i, 0)),
                  pl.BlockSpec((bn, k), lambda j, i: (j + off, 0)),
                  pl.BlockSpec((bm, bn), lambda j, i: (i, j + off))],
        out_specs=pl.BlockSpec((bm, bn), lambda j, i: (i, j)),
        out_shape=jax.ShapeDtypeStruct((m, n), BF),
        cost_estimate=_cost(m, k, n), compiler_params=_params(2))(g, w, z)


def _back_body(sub, a_ref, b_ref, wa_ref, wb_ref, r_ref, *refs):
    o_ref = refs[-1]
    for i in range(a_ref.shape[0] // sub):
        s = pl.ds(i * sub, sub)
        acc = lax.dot_general(a_ref[s, :], wa_ref[...], NT, preferred_element_type=F32)
        acc += lax.dot_general(b_ref[s, :], wb_ref[...], NT, preferred_element_type=F32)
        o_ref[s, :] = (acc + r_ref[s, :].astype(F32)).astype(BF)


def back(a, b, w, r, pieces=1, piece=0, into=None, bm=512, sub=256):
    m, k = a.shape
    n = w.shape[0]
    steps = m // bm // pieces
    off = piece * steps
    rows = pl.BlockSpec((bm, k), lambda i: (i + off, 0))
    out = pl.BlockSpec((bm, n), lambda i: (i + off, 0))
    extra = [] if into is None else [into]
    return pl.pallas_call(
        functools.partial(_back_body, sub), grid=(steps,),
        in_specs=[rows, rows, pl.BlockSpec((n, k), lambda i: (0, 0)), pl.BlockSpec((n, k), lambda i: (0, 1)), out]
        + [pl.BlockSpec(memory_space=pl.ANY)] * len(extra),
        out_specs=out, out_shape=jax.ShapeDtypeStruct((m, n), BF),
        input_output_aliases={5: 0} if extra else {},
        cost_estimate=_cost(m // pieces, 2 * k, n), compiler_params=_params(1))(a, b, w, w, r, *extra)


def _grad_body(at_ref, a_ref, b_ref, *refs):
    s = lax.dot_general(a_ref[...], b_ref[...], TN, preferred_element_type=F32)
    if len(refs) == 1:
        refs[0][...] = s
        return
    r_ref, o_ref, first_ref, second_ref = refs
    o_ref[...] = s + r_ref[...]
    part = first_ref.shape[1]
    far_j, far_k = 1 - at_ref[1], 1 - at_ref[2]
    if first_ref.shape[0] == 2:
        for i in range(2):
            first_ref[i] = o_ref[pl.ds(pl.multiple_of((far_j * 2 + i) * 2 * part, 8), part), :]
            second_ref[i] = o_ref[pl.ds(pl.multiple_of((i * 2 + far_k) * 2 * part + part, 8), part), :]
    else:
        i = pl.program_id(0)

        @pl.when(i // 2 == far_j)
        def _():
            first_ref[0] = o_ref[:part, :]

        @pl.when(i % 2 == far_k)
        def _():
            second_ref[0] = o_ref[part:, :]


def grad(at, a, b, start, cols, bm, bn, mib, recv=None):
    k = a.shape[0]
    rows = a.shape[1] // 2
    tiles = rows // bm
    out = pl.BlockSpec((bm, bn), lambda i, j, t: (i, j))
    shape = jax.ShapeDtypeStruct((rows, cols), F32)
    specs = [pl.BlockSpec((k, bm), lambda i, j, t: (0, i + t[0] * tiles)),
             pl.BlockSpec((pl.Element(k), pl.Element(bn)), lambda i, j, t: (0, pl.multiple_of(start + j * bn, 128)))]
    args = [at, a, b]
    if recv is not None:
        specs.append(out)
        args.append(recv)
        if tiles == 1:
            one = two = pl.BlockSpec((2, rows // 8, bn), lambda i, j, t: (0, 0, j))
        else:
            one = pl.BlockSpec((1, rows // 8, bn), lambda i, j, t: (jnp.clip(i - 2 * (1 - t[1]), 0, 1), 0, j))
            two = pl.BlockSpec((1, rows // 8, bn), lambda i, j, t: (i // 2, 0, j))
        out = [out, one, two]
        shape = [shape] + [jax.ShapeDtypeStruct((2, rows // 8, cols), F32)] * 2
    return pl.pallas_call(
        _grad_body,
        grid_spec=pltpu.PrefetchScalarGridSpec(num_scalar_prefetch=1, grid=(tiles, cols // bn), in_specs=specs,
                                               out_specs=out),
        out_shape=shape, cost_estimate=_cost(rows, k, cols), compiler_params=_params(2, mib))(*args)


def _copy_body(*refs):
    refs[-1][...] = refs[0][...]


def copy(w, shape=None, half=0, into=None, steps=5):
    rows, cols = w.shape
    block = pl.BlockSpec((rows // steps, cols), lambda i: (i, 0))
    return pl.pallas_call(
        _copy_body, grid=(steps,),
        in_specs=[block] + ([] if into is None else [pl.BlockSpec(memory_space=pl.ANY)]),
        out_specs=pl.BlockSpec((rows // steps, cols), lambda i: (i, half)),
        out_shape=jax.ShapeDtypeStruct(shape or w.shape, w.dtype),
        input_output_aliases={} if into is None else {1: 0},
        cost_estimate=pl.CostEstimate(flops=rows * cols * 64, bytes_accessed=4 * rows * cols, transcendentals=0),
        compiler_params=_params(1))(w, *([] if into is None else [into]))


class Chunk:
    def __init__(self, parts):
        s, *self.out = parts
        self.j, self.k = lax.axis_index("dy"), lax.axis_index("dz")
        rows, cols = s.shape
        self.size = rows // 8, cols
        self.s = s.reshape(2, 2, 2, rows // 8, cols)

    def cut(self, j, k, part, n):
        r, c = self.size
        return lax.dynamic_slice(self.s, (j, k, part, 0, 0), (*n, 1, r, c)).reshape(n[0] * n[1], r, c)

    def send(self, stage, vals):
        axes = ("dy", "dz") if stage == 1 else ("dz", "dy")
        self.flight = []
        for v, ax in zip(vals, axes):
            self.flight.append(lax.ppermute(v, ax, SWAP))

    def second(self, vals):
        j, k = self.j, self.k
        self.ra, self.rb = vals
        pick = lax.dynamic_index_in_dim
        self.out = (self.cut(j, 1 - k, 0, (1, 1)) + pick(self.ra, 1 - k, 0),
                    self.cut(1 - j, k, 1, (1, 1)) + pick(self.rb, 1 - j, 0))

    def total(self, vals):
        j, k = self.j, self.k
        pick = lax.dynamic_index_in_dim
        a = self.cut(j, k, 0, (1, 1)) + pick(self.ra, k, 0) + vals[0]
        b = self.cut(j, k, 1, (1, 1)) + pick(self.rb, j, 0) + vals[1]
        return jnp.concatenate([a[0], b[0]], axis=0)


def solution(mesh):
    ndy, ndz = mesh.shape["dy"], mesh.shape["dz"]
    n = mesh.shape["dx"] * ndy * ndz

    def dot(a, b):
        return jnp.dot(a, b, preferred_element_type=F32)

    def local(x, g, w1, w2, w3, w4, m1, m2, m3, m4):
        core = lax.axis_index("dx")
        spot = [core, lax.axis_index("dy"), lax.axis_index("dz")]
        own = jnp.stack(spot).astype(jnp.int32)
        other = jnp.stack([1 - core, *spot[1:]]).astype(jnp.int32)
        tall = dict(a=dict(start=0, cols=512, bm=640, bn=512), b=dict(start=512, cols=768, bm=640, bn=768))
        whole = dict(a=dict(start=0, cols=2560, bm=640, bn=512))
        whole["b"] = whole["a"]

        def gate(*vals):
            return lax.optimization_barrier(vals)

        def send(s):
            return lax.ppermute(s, "dx", SWAP)

        def part(layer, which, a, b, recv=None):
            half, _ = (other, "p") if recv is None else (own, "o")
            sizes = (tall if layer in "24" else whole)[which]
            return grad(half, a, b, **sizes, mib=38 if layer == "4" else 60, recv=recv)

        def update(w, m, s, start=0):
            rows, cols = s.shape
            idx = (core * ndy + lax.axis_index("dy")) * ndz + lax.axis_index("dz")
            m_new = MU * lax.slice_in_dim(m, start, start + cols, axis=1) + s / n
            w_loc = lax.dynamic_slice(w, (idx * rows, start), (rows, cols)).astype(F32)
            return (w_loc - LR * m_new).astype(BF), m_new

        def both(ca, cb, vals):
            return jnp.concatenate([ca.total(vals[:2]), cb.total(vals[2:])], axis=1)

        def gather(w):
            return lax.all_gather(w, DATA, axis=0, tiled=True)

        z1, h1 = zh(x, w1)
        h2 = (dot(h1, w2) + x.astype(F32)).astype(BF)
        z3, h3 = zh(h2, w3)

        h3, p = gate(h3, part("4", "a", h3, g))
        d4a = send(p)
        h3, p = gate(h3, part("4", "b", h3, g))
        d4b = send(p)
        c4a = Chunk(part("4", "a", h3, g, d4a))
        h3, *v = gate(h3, *c4a.out)
        c4a.send(1, v)
        c4b = Chunk(part("4", "b", h3, g, d4b))
        g_, *v = gate(g, *c4b.out)
        c4b.send(1, v)
        g_, *v = gate(g_, *c4a.flight)
        c4a.second(v)
        g_, *v = gate(g_, *c4a.out)
        c4a.send(2, v)
        dza = dz_half(g_, w4, z3, 0)
        dza, *v = gate(dza, *c4b.flight)
        c4b.second(v)
        dza, *v = gate(dza, *c4b.out)
        c4b.send(2, v)
        g_, p = gate(g_, part("3", "a", h2, dza))
        d3a = send(p)
        g_, *v = gate(g_, *c4a.flight, *c4b.flight)
        w4l, m4n = update(w4, m4, both(c4a, c4b, v))
        g_, w4l, m4n = gate(g_, w4l, m4n)
        w4g = gather(w4l)
        dzb = dz_half(g_, w4, z3, 1)
        dza, p = gate(dza, part("3", "b", h2, dzb))
        d3b = send(p)
        c3a = Chunk(part("3", "a", h2, dza, d3a))
        dzb, *v = gate(dzb, *c3a.out)
        c3a.send(1, v)
        c3b = Chunk(part("3", "b", h2, dzb, d3b))
        dzb, *v = gate(dzb, *c3b.out)
        c3b.send(1, v)
        top = back(dza, dzb, w3, g, 2, 0)
        top, *v = gate(top, *c3a.flight)
        c3a.second(v)
        top, *v = gate(top, *c3a.out)
        c3a.send(2, v)
        dh2 = back(dza, dzb, w3, g, 2, 1, top)
        dh2, *v = gate(dh2, *c3b.flight)
        c3b.second(v)
        dh2, *v = gate(dh2, *c3b.out)
        c3b.send(2, v)
        dh2, p = gate(dh2, part("2", "a", h1, dh2))
        d2a = send(p)
        dh2, *v = gate(dh2, *c3a.flight, *c3b.flight)
        w3l, m3n = update(w3, m3, both(c3a, c3b, v))
        dh2, w3l, m3n = gate(dh2, w3l, m3n)
        w3g = gather(w3l)
        dh2, p = gate(dh2, part("2", "b", h1, dh2))
        d2b = send(p)
        c2a = Chunk(part("2", "a", h1, dh2, d2a))
        dh2, *v = gate(dh2, *c2a.out)
        c2a.send(1, v)
        c2b = Chunk(part("2", "b", h1, dh2, d2b))
        dh2, *v = gate(dh2, *c2b.out)
        c2b.send(1, v)
        dza = dz_half(dh2, w2, z1, 0)
        p = part("1", "a", x, dza)
        dh2, p, *v = gate(dh2, p, *c2a.flight, *c2b.flight)
        d1a = send(p)
        c2a.second(v[:2])
        c2b.second(v[2:])
        dh2, *v = gate(dh2, *c2a.out, *c2b.out)
        c2a.send(2, v[:2])
        c2b.send(2, v[2:])
        dzb = dz_half(dh2, w2, z1, 1)
        dzb, *v = gate(dzb, *c2a.flight, *c2b.flight)
        w2l, m2n = update(w2, m2, both(c2a, c2b, v))
        dzb, w2l, m2n = gate(dzb, w2l, m2n)
        w2g = gather(w2l)
        c1a = Chunk(part("1", "a", x, dza, d1a))
        dzb, *v = gate(dzb, *c1a.out)
        c1a.send(1, v)
        dza, w4g, p = gate(dza, w4g, part("1", "b", x, dzb))
        d1b = send(p)
        w4n = copy(w4g)
        dzb, d1b, w4n = gate(dzb, d1b, w4n)
        c1b = Chunk(part("1", "b", x, dzb, d1b))
        dzb, *v = gate(dzb, *c1b.out)
        c1b.send(1, v)
        dzb, *v = gate(dzb, *c1a.flight)
        c1a.second(v)
        dzb, *v = gate(dzb, *c1a.out)
        c1a.send(2, v)
        top = back(dza, dzb, w1, dh2, 2, 0)
        top, *v = gate(top, *c1a.flight)
        wa, ma = update(w1, m1, c1a.total(v))
        top, wa = gate(top, wa)
        ga = gather(wa)
        top, w3g = gate(top, w3g)
        w3n = copy(w3g)
        top, w3n, w2g, *v = gate(top, w3n, w2g, *c1b.flight)
        c1b.second(v)
        top, w2g, *v = gate(top, w2g, *c1b.out)
        c1b.send(2, v)
        w2n = copy(w2g)
        top, w2n, *v = gate(top, w2n, *c1b.flight)
        wb, mb = update(w1, m1, c1b.total(v), start=wa.shape[1])
        top, wb = gate(top, wb)
        gb = gather(wb)
        dx = back(dza, dzb, w1, dh2, 2, 1, top)
        dx, ga = gate(dx, ga)
        half = copy(ga, w1.shape, 0)
        half, gb = gate(half, gb)
        w1n = copy(gb, w1.shape, 1, half)
        m1n = jnp.concatenate([ma, mb], axis=1)
        return (dx, w1n, w2n, w3n, w4n, m1n, m2n, m3n, m4n)

    row, rep = P(DATA, None), P()
    return jax.shard_map(local, mesh=mesh,
                         in_specs=(row, row, rep, rep, rep, rep, row, row, row, row),
                         out_specs=(row, rep, rep, rep, rep, row, row, row, row),
                         check_vma=False)
```
